256 devices in a mesh: vocab: 64 (over y, z, core), batch: 4 (over x).
Axes of the slice: x: 4, y: 4, z: 8, core: 2. Of those that a mesh axis runs over, the one named last changes fastest.
Arguments:
- latent_activation: bfloat16 [3, 512, 6144], P(None, ('batch', 'vocab')), parts along dimension 1, may hold values from -6 to 6
- readout_matrix: bfloat16 [6144, 32768], P(None, 'vocab'), may hold values from -0.078125 to 0.078125
- caller_additive_shift: float32 [512, 32768], P('batch', 'vocab'), parts along dimension 0, may hold values from -4 to 600
- uniform_jitter: float32 [3, 512, 32768], P(None, 'batch', 'vocab'), parts along dimension 1, may hold values from 0.001 to 0.999
- context_word_indices: int32 [512, 256], P('batch'), parts along dimension 0, may hold values from 0 to 32767
- emitted_word_indices: int32 [512, 3], P('batch'), parts along dimension 0, may hold values from 0 to 32767
- heat_factor: float32 [512], P('batch'), parts along dimension 0, may hold values from 0.7 to 1.4
- recurrence_charge: float32 [512], P('batch'), parts along dimension 0, may hold values from 1.05 to 1.3
- appearance_charge: float32 [512], P('batch'), parts along dimension 0, may hold values from 0 to 1
- occurrence_charge: float32 [512], P('batch'), parts along dimension 0, may hold values from 0 to 1
Outputs:
- perturbed_max: float32 [3, 512], P(None, 'batch'), parts along dimension 1
- target_logprob: float32 [3, 512], P(None, 'batch'), parts along dimension 1
- last_logprobs: float32 [512, 32768], P('batch', 'vocab'), parts along dimension 0
The draws below stay inside these ranges and needn't reach their ends.
There are 4 independent parts, one for each index of `batch`. The reference program is written for one: setup_inputs(seed, part) draws one part's arguments, and reference() takes and returns one part's arrays. A program takes and returns all parts, laid end to end along the dimension named above; an argument that names none is the same for every part. Nothing has to cross between parts.
All inputs are finite; a program needn't handle non-finite values.
Results may differ from the reference program's by a relative error of at most 0.0003.
Values may be sent and summed in bfloat16 or wider, within the bound.
No kernel may reach another device: no remote copies, remote signals or barrier semaphores. Data moves between devices by JAX's collectives and lax.ppermute only.
A program may use at most 64 MiB of HBM per device.

```python
import math
import jax
import jax.numpy as jnp
import numpy as np

D = 6144
V = 32768
BATCH_MEMBERS = 128
P_SIZE = 256
STEPS = 3


def draw_caller_additive_shift(key, part):
    base = jnp.clip(jax.random.normal(jax.random.fold_in(key, 11), (BATCH_MEMBERS, V), jnp.float32), -4.0, 4.0)
    return base


def set_ends(drawn, stream_key, least, top_value):
    dims = drawn.shape
    spot = [jax.random.randint(jax.random.fold_in(stream_key, axis), (), 0, dims[axis]) for axis in range(len(dims))]
    drawn = drawn.at[tuple(spot)].set(least)
    longest = dims.index(max(dims))
    spot[longest] = (spot[longest] + 1) % dims[longest]
    return drawn.at[tuple(spot)].set(top_value)


def shard_levels(key, shape, shards, smallest, largest):
    def one(axis_at, blocks):
        steps = jax.random.uniform(jax.random.fold_in(jax.random.fold_in(key, 6), axis_at), (blocks,), jnp.float32, smallest / len(shards), largest / len(shards))
        return jnp.repeat(jnp.exp(steps), shape[axis_at] // blocks).reshape((-1,) + (1,) * (len(shape) - axis_at - 1))

    level = one(*shards[0])
    for cut in shards[1:]:
        level = level * one(*cut)
    return level


def rank_table(amount, skew):
    loads = [(1 << 20) // math.isqrt(grade ** skew) + 1 for grade in range(1, amount + 1)]
    deviation = 1 + sum(loads) // (1 << 30)
    return np.cumsum(np.array([max(1, weight // deviation) for weight in loads]))


def skewed_ids(rng, shape, count, skew):
    listing = rank_table(count, skew)
    lot = jax.random.randint(jax.random.fold_in(rng, 1), shape, 0, int(listing[count - 1]))
    rank = jnp.searchsorted(jnp.asarray(listing, jnp.int32), lot, side="right")
    return jax.random.permutation(jax.random.fold_in(rng, 2), count)[rank].astype(jnp.int32)


def noise(rng, dims, deviation, reach, shards=(), kind=jnp.bfloat16):
    entries = jax.random.normal(rng, dims, jnp.float32) * deviation
    if len(shards) > 0:
        entries = shard_levels(rng, dims, shards, -0.22, 0.18) * entries
    return jnp.clip(entries, min=-reach, max=reach).astype(kind)


def setup_inputs(seed: int = 0, part: int = 0) -> dict:
    keys = jax.random.split(jax.random.key(seed), 11)
    part_keys = jax.random.split(jax.random.fold_in(keys[10], part), 11)
    latent_activation = noise(part_keys[0], (STEPS, BATCH_MEMBERS, D), 1.0, 6.0, ((1, 64),))
    readout_matrix = noise(keys[1], (D, V), D ** -0.5, 0.078125, ((1, 64),))
    caller_additive_shift = draw_caller_additive_shift(jax.random.fold_in(jax.random.fold_in(keys[10], part), 71), part)
    uniform_jitter = jnp.clip(0.001 + 0.998 * jax.random.uniform(part_keys[3], (STEPS, BATCH_MEMBERS, V), jnp.float32) ** shard_levels(part_keys[3], (STEPS, BATCH_MEMBERS, V), ((2, 64),), -0.2, 0.2), 0.001, 0.999)
    context_word_indices = set_ends(skewed_ids(part_keys[4], (BATCH_MEMBERS, P_SIZE), V, 2), jax.random.fold_in(part_keys[4], 3), 0, V - 1).astype(jnp.int32)
    emitted_word_indices = set_ends(skewed_ids(part_keys[5], (BATCH_MEMBERS, STEPS), V, 2), jax.random.fold_in(part_keys[5], 3), 0, V - 1).astype(jnp.int32)
    heat_factor = jnp.clip(jnp.exp(jax.random.uniform(part_keys[6], (BATCH_MEMBERS,), jnp.float32, math.log(0.7), math.log(1.4))), 0.7, 1.4)
    recurrence_charge = jnp.clip(jnp.exp(jax.random.uniform(part_keys[7], (BATCH_MEMBERS,), jnp.float32, math.log(1.05), math.log(1.3))), 1.05, 1.3)
    appearance_charge = jnp.clip(jax.random.uniform(part_keys[8], (BATCH_MEMBERS,), jnp.float32, 0.0, 1.0), 0.0, 1.0)
    occurrence_charge = jnp.clip(jax.random.uniform(part_keys[9], (BATCH_MEMBERS,), jnp.float32, 0.0, 1.0), 0.0, 1.0)
    return dict(latent_activation=latent_activation, readout_matrix=readout_matrix, caller_additive_shift=caller_additive_shift, uniform_jitter=uniform_jitter, context_word_indices=context_word_indices, emitted_word_indices=emitted_word_indices, heat_factor=heat_factor, recurrence_charge=recurrence_charge, appearance_charge=appearance_charge, occurrence_charge=occurrence_charge)


def enforce_repeat_charges(plain_energies, word_tallies, caller_additive_shift, heat_factor, recurrence_charge, appearance_charge, occurrence_charge):
    seen = word_tallies > 0
    counted = word_tallies.astype(jnp.float32)
    biased = plain_energies + caller_additive_shift
    repeat = recurrence_charge[:, None]
    cooled_energies = jnp.where(seen, jnp.where(biased > 0, biased / repeat, biased * repeat), biased)
    cooled_energies = cooled_energies - occurrence_charge[:, None] * counted - appearance_charge[:, None] * seen.astype(jnp.float32)
    return cooled_energies / heat_factor[:, None]


def reference(latent_activation, readout_matrix, caller_additive_shift, uniform_jitter, context_word_indices, emitted_word_indices, heat_factor, recurrence_charge, appearance_charge, occurrence_charge):
    batch_rows = jnp.arange(BATCH_MEMBERS, dtype=jnp.int32)
    word_tallies = jnp.zeros((BATCH_MEMBERS, V), jnp.int32).at[batch_rows[:, None], context_word_indices].add(1)
    plain_energies = jnp.dot(latent_activation.reshape(STEPS * BATCH_MEMBERS, D), readout_matrix, preferred_element_type=jnp.float32).reshape(STEPS, BATCH_MEMBERS, V)
    best_list = []
    target_list = []
    last = None
    for generation_moment in range(STEPS):
        word_energies = enforce_repeat_charges(plain_energies[generation_moment], word_tallies, caller_additive_shift, heat_factor, recurrence_charge, appearance_charge, occurrence_charge)
        gumbel = -jnp.log(-jnp.log(uniform_jitter[generation_moment]))
        best_list.append(jnp.max(word_energies + gumbel, axis=1))
        top = jnp.max(word_energies, axis=1)
        normalizer = top + jnp.log(jnp.sum(jnp.exp(word_energies - top[:, None]), axis=1))
        taken = emitted_word_indices[:, generation_moment]
        target_score = jnp.take_along_axis(word_energies, taken[:, None], axis=1)[:, 0]
        target_list.append(target_score - normalizer)
        last = word_energies - normalizer[:, None]
        word_tallies = word_tallies.at[batch_rows, taken].add(1)
    return jnp.stack(best_list), jnp.stack(target_list), last
```

```python
import functools

import jax
import jax.numpy as jnp
from jax import lax
from jax.experimental import pallas as pl
from jax.experimental.pallas import tpu as pltpu
from jax.sharding import PartitionSpec as P

NY, NZ, NC = 4, 8, 2
NV = NY * NZ * NC
LANES = 128


def device_of(y, z, c):
    return ((y % NY) * NZ + z % NZ) * NC + c % NC


def moved(array, dy=0, dz=0, dc=0):
    pairs = [
        (device_of(y, z, c), device_of(y + dy, z + dz, c + dc))
        for y in range(NY)
        for z in range(NZ)
        for c in range(NC)
    ]
    return lax.ppermute(array, "vocab", pairs)


def prologue_kernel(base_ref, ctx_ref, jitter_ref, counts_ref, gumbel_ref, found_ref):
    batch_rows, length = ctx_ref.shape
    width = counts_ref.shape[1]
    blocks = width // LANES
    base = base_ref[0]
    block_ids = lax.broadcasted_iota(jnp.int32, (8, length), 0)
    lane_ids = lax.broadcasted_iota(jnp.int32, (LANES, length), 0)

    def count_row(b):
        local = ctx_ref[pl.ds(b, 1), :] - base
        high = lax.shift_right_arithmetic(local, 7)
        low = jnp.bitwise_and(local, LANES - 1)
        lhs = (block_ids == high).astype(jnp.float32).astype(jnp.bfloat16)
        rhs = (lane_ids == low).astype(jnp.float32).astype(jnp.bfloat16)
        return lax.dot_general(lhs, rhs, (((1,), (1,)), ((), ())), preferred_element_type=jnp.float32)

    def count_rows(i, carry):
        rows = pl.ds(pl.multiple_of(i * 8, 8), 8)
        for j in range(8):
            found_ref[8 * j : 8 * j + 8, :] = count_row(i * 8 + j)
        for k in range(blocks):
            counts_ref[rows, k * LANES : (k + 1) * LANES] = found_ref[pl.ds(k, 8, stride=8), :]
        return carry

    lax.fori_loop(0, batch_rows // 8, count_rows, 0)

    def gumbel_rows(i, carry):
        rows = pl.ds(pl.multiple_of(i * 8, 8), 8)
        for t in range(jitter_ref.shape[0]):
            gumbel_ref[t, rows, :] = -jnp.log(-jnp.log(jitter_ref[t, rows, :]))
        return carry

    lax.fori_loop(0, batch_rows // 8, gumbel_rows, 0)


def prologue(base, ctx, jitter, width):
    batch_rows = ctx.shape[0]
    vmem = pl.BlockSpec(memory_space=pltpu.VMEM)
    return pl.pallas_call(
        prologue_kernel,
        out_shape=(
            jax.ShapeDtypeStruct((batch_rows, width), jnp.float32),
            jax.ShapeDtypeStruct(jitter.shape, jnp.float32),
        ),
        in_specs=[pl.BlockSpec(memory_space=pltpu.SMEM), vmem, vmem],
        out_specs=(vmem, vmem),
        scratch_shapes=[pltpu.VMEM((8 * 8, LANES), jnp.float32)],
        compiler_params=pltpu.CompilerParams(vmem_limit_bytes=16 * 2**20),
        cost_estimate=pl.CostEstimate(flops=5_000_000_000, bytes_accessed=2_000_000, transcendentals=800_000),
        name="prologue",
    )(base, ctx, jitter)


def epilogue_kernel(places, steps, idx_ref, *refs):
    pieces = refs[: len(places)]
    counts_ref, shift_ref, gumbel_ref, emitted_ref, par_ref = refs[len(places) : len(places) + 5]
    scores_ref, stats_ref, logits_ref, columns_ref, ring_ref = refs[len(places) + 5 :]
    batch_rows, width = counts_ref.shape
    y, z, c, base = idx_ref[0], idx_ref[1], idx_ref[2], idx_ref[3]
    where_is = {place: (ref, g) for ref, group in zip(pieces, places) for g, place in enumerate(group)}
    pair = 2
    ring = NZ * NC * pair
    for k, dy in enumerate((0, -1, 1, 2)):
        yy = jnp.bitwise_and(y + (dy + NY), NY - 1)
        for t in range(steps):
            for dz in range(NZ):
                block = []
                for dc in range(NC):
                    ref, g = where_is[dz, dc]
                    at = ((g * NY + k) * steps + t) * pair
                    block.append(ref[at : at + pair, :])
                row = dz * NC * pair + 8
                ring_ref[k * steps + t, row : row + pair, :] = jnp.where(c == 0, block[0], block[1])
                ring_ref[k * steps + t, row + pair : row + 2 * pair, :] = jnp.where(c == 0, block[1], block[0])
            ring_ref[k * steps + t, 4:8, :] = ring_ref[k * steps + t, ring + 4 : ring + 8, :]
            for i in range(ring // 8):
                even = ring_ref[k * steps + t, 8 * i + 8 : 8 * i + 16, :]
                odd = ring_ref[k * steps + t, 8 * i + 4 : 8 * i + 12, :]
                tile = jnp.bitwise_and(i + lax.shift_right_logical(z, 1), ring // 8 - 1)
                at = pl.multiple_of(yy * ring + tile * 8, 8)
                logits_ref[t, pl.ds(at, 8), :] = jnp.where(jnp.bitwise_and(z, 1) == 1, odd, even)

    rows_at_once = 32
    lane = lax.broadcasted_iota(jnp.int32, (rows_at_once, width), 1) + base

    def some_rows(i, carry):
        rows = pl.ds(pl.multiple_of(i * rows_at_once, rows_at_once), rows_at_once)
        par = par_ref[rows, :]
        repeat, unrepeat = par[:, 0:1], par[:, 1:2]
        present, frequent, cooling = par[:, 2:3], par[:, 3:4], par[:, 4:5]
        emitted = emitted_ref[rows, :]
        counts = counts_ref[rows, :]
        shift = shift_ref[rows, :]
        for t in range(steps):
            biased = logits_ref[t, rows, :] + shift
            seen = counts > 0
            factor = jnp.where(biased > 0, unrepeat, repeat)
            charged = biased * jnp.where(seen, factor, 1.0)
            charged = charged - frequent * counts - jnp.where(seen, present, 0.0)
            scores = charged * cooling
            hit = lane == emitted[:, t : t + 1]
            top = jnp.max(scores, axis=1, keepdims=True)
            total = jnp.sum(jnp.exp(scores - top), axis=1, keepdims=True)
            columns_ref[rows, 3 * t : 3 * t + 1] = top + jnp.log(total)
            columns_ref[rows, 3 * t + 1 : 3 * t + 2] = jnp.max(
                scores + gumbel_ref[t, rows, :], axis=1, keepdims=True
            )
            columns_ref[rows, 3 * t + 2 : 3 * t + 3] = jnp.sum(
                jnp.where(hit, scores, 0.0), axis=1, keepdims=True
            )
            if t == steps - 1:
                scores_ref[rows, :] = scores
            counts = counts + jnp.where(hit, 1.0, 0.0)
        return carry

    lax.fori_loop(0, batch_rows // rows_at_once, some_rows, 0)
    turned = columns_ref[...].T
    for k in range(3 * steps):
        stats_ref[0:1, k * batch_rows : (k + 1) * batch_rows] = turned[k : k + 1, :]


def epilogue(places, idx, pieces, counts, shift, gumbel, emitted, par):
    steps, batch_rows, width = gumbel.shape
    vmem = pl.BlockSpec(memory_space=pltpu.VMEM)
    return pl.pallas_call(
        functools.partial(epilogue_kernel, places, steps),
        out_shape=(
            jax.ShapeDtypeStruct((batch_rows, width), jnp.float32),
            jax.ShapeDtypeStruct((1, 3 * steps * batch_rows), jnp.float32),
        ),
        in_specs=[pl.BlockSpec(memory_space=pltpu.SMEM)] + [vmem] * (len(pieces) + 5),
        out_specs=(vmem, vmem),
        scratch_shapes=[
            pltpu.VMEM((steps, batch_rows, width), jnp.float32),
            pltpu.VMEM((batch_rows, LANES), jnp.float32),
            pltpu.VMEM((NY * steps, NZ * NC * 2 + 8, width), jnp.float32),
        ],
        compiler_params=pltpu.CompilerParams(vmem_limit_bytes=16 * 2**20),
        cost_estimate=pl.CostEstimate(flops=2_000_000_000, bytes_accessed=4_000_000, transcendentals=200_000),
        name="epilogue",
    )(idx, *pieces, counts, shift, gumbel, emitted, par)


def gathered_products(own, matrix):
    dim = own.shape[-1]

    def product(bundles):
        rows = [b.reshape(-1, dim) for b in bundles]
        return jnp.dot(jnp.concatenate(rows, 0), matrix, preferred_element_type=jnp.float32)

    column = [own, moved(own, dy=1), moved(own, dy=-1), moved(own, dy=2)]
    bundle = jnp.concatenate(column, 0)
    products = [product([bundle, moved(bundle, dc=1)])]
    places = [[(0, 0), (0, 1)]]
    up, down = bundle, bundle
    for step in range(1, NZ // 2):
        up, down = moved(up, dz=1), moved(down, dz=-1)
        products.append(product([up, down, moved(up, dc=1), moved(down, dc=1)]))
        places.append([(NZ - step, 0), (step, 0), (NZ - step, 1), (step, 1)])
    up, down = moved(up[..., : dim // 2], dz=1), moved(down[..., dim // 2 :], dz=-1)
    far = jnp.concatenate([up, down], -1)
    products.append(product([far, moved(far, dc=1)]))
    places.append([(NZ // 2, 0), (NZ // 2, 1)])
    return products, places


def per_device(
    latent_activation,
    readout_matrix,
    caller_additive_shift,
    uniform_jitter,
    context_word_indices,
    emitted_word_indices,
    heat_factor,
    recurrence_charge,
    appearance_charge,
    occurrence_charge,
):
    width = readout_matrix.shape[1]
    steps, batch_rows = uniform_jitter.shape[:2]
    place = lax.axis_index("vocab")
    base = place * width
    idx = jnp.stack([place // (NZ * NC), (place // NC) % NZ, place % NC, base]).astype(jnp.int32)
    products, places = gathered_products(latent_activation, readout_matrix)
    counts, gumbel = prologue(idx[3:], context_word_indices, uniform_jitter, width)
    par = jnp.stack(
        [
            recurrence_charge,
            1.0 / recurrence_charge,
            appearance_charge,
            occurrence_charge,
            1.0 / heat_factor,
        ],
        axis=1,
    )
    scores, stats = epilogue(
        places, idx, products, counts, caller_additive_shift, gumbel, emitted_word_indices, par
    )
    everyone = lax.all_to_all(
        jnp.broadcast_to(stats[None], (NV, *stats.shape)), "vocab", 0, 0, tiled=True
    ).reshape(NV, steps, 3, batch_rows)
    top = jnp.max(everyone[:, :, 0], axis=0)
    normalizer = top + jnp.log(jnp.sum(jnp.exp(everyone[:, :, 0] - top), axis=0))
    best = jnp.max(everyone[:, :, 1], axis=0)
    target = jnp.sum(everyone[:, :, 2], axis=0)
    return best, target - normalizer, scores - normalizer[-1][:, None]


def solution(mesh):
    in_specs = (
        P(None, ("batch", "vocab"), None),
        P(None, "vocab"),
        P("batch", "vocab"),
        P(None, "batch", "vocab"),
        P("batch", None),
        P("batch", None),
        P("batch"),
        P("batch"),
        P("batch"),
        P("batch"),
    )
    out_specs = (P(None, "batch"), P(None, "batch"), P("batch", "vocab"))
    return jax.shard_map(
        per_device, mesh=mesh, in_specs=in_specs, out_specs=out_specs, check_vma=False
    )
```

```python
import functools

import jax
import jax.numpy as jnp
from jax import lax
from jax.experimental import pallas as pl
from jax.experimental.pallas import tpu as pltpu
from jax.sharding import PartitionSpec as P


NY, NZ, NC = 4, 8, 2
NV = NY * NZ * NC
LANES = 128


def device_of(y, z, c):
    return ((y % NY) * NZ + z % NZ) * NC + c % NC


def moved(array, dy=0, dz=0, dc=0):
    pairs = [
        (device_of(y, z, c), device_of(y + dy, z + dz, c + dc))
        for y in range(NY)
        for z in range(NZ)
        for c in range(NC)
    ]
    return lax.ppermute(array, "vocab", pairs)


def prologue_kernel(ctx_hbm, jitter_hbm, emitted_ref, repeat_ref, present_ref, frequent_ref, heat_ref,
                    counts_ref, gumbel_ref, par_ref, ctx_ref, found_ref, rows_ref, ctx_sem, jitter_sem):
    batch_rows, length = ctx_ref.shape
    width = counts_ref.shape[1]
    steps = gumbel_ref.shape[0]
    blocks = width // LANES
    base = lax.axis_index("vocab") * width
    ctx_copy = pltpu.make_async_copy(ctx_hbm, ctx_ref, ctx_sem)
    jitter_copy = pltpu.make_async_copy(jitter_hbm, gumbel_ref, jitter_sem)
    ctx_copy.start()
    jitter_copy.start()

    rows_ref[...] = jnp.zeros_like(rows_ref)
    rows_ref[0:1, :] = repeat_ref[...]
    rows_ref[1:2, :] = 1.0 / repeat_ref[...]
    rows_ref[2:3, :] = present_ref[...]
    rows_ref[3:4, :] = frequent_ref[...]
    rows_ref[4:5, :] = 1.0 / heat_ref[...]
    rows_ref[8 : 8 + steps, :] = (emitted_ref[...] - base).astype(jnp.float32)
    par_ref[...] = rows_ref[...].T

    block_ids = lax.broadcasted_iota(jnp.int32, (8, length), 0)
    lane_ids = lax.broadcasted_iota(jnp.int32, (LANES, length), 0)

    def count_row(b):
        local = ctx_ref[pl.ds(b, 1), :] - base
        high = lax.shift_right_arithmetic(local, 7)
        low = jnp.bitwise_and(local, LANES - 1)
        lhs = (block_ids == high).astype(jnp.float32).astype(jnp.bfloat16)
        rhs = (lane_ids == low).astype(jnp.float32).astype(jnp.bfloat16)
        return lax.dot_general(lhs, rhs, (((1,), (1,)), ((), ())), preferred_element_type=jnp.float32)

    def count_rows(i, carry):
        rows = pl.ds(pl.multiple_of(i * 8, 8), 8)
        for j in range(8):
            found_ref[8 * j : 8 * j + 8, :] = count_row(i * 8 + j)
        for k in range(blocks):
            counts_ref[rows, k * LANES : (k + 1) * LANES] = found_ref[pl.ds(k, 8, stride=8), :]
        return carry

    ctx_copy.wait()
    lax.fori_loop(0, batch_rows // 8, count_rows, 0)

    def gumbel_rows(i, carry):
        rows = pl.ds(pl.multiple_of(i * 8, 8), 8)
        for t in range(steps):
            gumbel_ref[t, rows, :] = -jnp.log(-jnp.log(gumbel_ref[t, rows, :]))
        return carry

    jitter_copy.wait()
    lax.fori_loop(0, batch_rows // 8, gumbel_rows, 0)


def prologue(ctx, jitter, emitted, repeat, present, frequent, heat):
    batch_rows, length = ctx.shape
    width = jitter.shape[-1]
    vmem = pl.BlockSpec(memory_space=pltpu.VMEM)
    anywhere = pl.BlockSpec(memory_space=pltpu.HBM)
    return pl.pallas_call(
        prologue_kernel,
        out_shape=(
            jax.ShapeDtypeStruct((batch_rows, width), jnp.float32),
            jax.ShapeDtypeStruct(jitter.shape, jnp.float32),
            jax.ShapeDtypeStruct((batch_rows, LANES), jnp.float32),
        ),
        in_specs=[anywhere] * 2 + [vmem] * 5,
        out_specs=(vmem,) * 3,
        scratch_shapes=[
            pltpu.VMEM((batch_rows, length), jnp.int32),
            pltpu.VMEM((8 * 8, LANES), jnp.float32),
            pltpu.VMEM((LANES, batch_rows), jnp.float32),
            pltpu.SemaphoreType.DMA,
            pltpu.SemaphoreType.DMA,
        ],
        compiler_params=pltpu.CompilerParams(vmem_limit_bytes=4 * 2**20),
        cost_estimate=pl.CostEstimate(flops=5_000_000_000, bytes_accessed=2_000_000, transcendentals=800_000),
        name="prologue",
    )(ctx, jitter, emitted, repeat, present, frequent, heat)


def product_kernel(groups, *refs):
    matrix_ref, out_ref, rows_ref = refs[sum(groups) :]
    depth = 1024
    first = 0
    for g, parts in enumerate(groups):
        at = 0
        for ref in refs[first : first + parts]:
            count, part = ref.shape
            rows_ref[g * count : (g + 1) * count, at : at + part] = ref[...]
            at += part
        first += parts

    def add(k, carry):
        at = pl.ds(pl.multiple_of(k * depth, depth), depth)
        out_ref[...] += jnp.dot(rows_ref[:, at], matrix_ref[at, :], preferred_element_type=jnp.float32)
        return carry

    out_ref[...] = jnp.zeros_like(out_ref)
    lax.fori_loop(0, rows_ref.shape[1] // depth, add, 0)


def product(groups, matrix):
    vmem = pl.BlockSpec(memory_space=pltpu.VMEM)
    dim, width = matrix.shape
    count = sum(group[0].shape[0] for group in groups)
    parts = [part for group in groups for part in group]
    return pl.pallas_call(
        functools.partial(product_kernel, [len(group) for group in groups]),
        out_shape=jax.ShapeDtypeStruct((count, width), jnp.float32),
        in_specs=[vmem] * (len(parts) + 1),
        out_specs=vmem,
        scratch_shapes=[pltpu.VMEM((count, dim), jnp.bfloat16)],
        compiler_params=pltpu.CompilerParams(vmem_limit_bytes=4 * 2**20),
        cost_estimate=pl.CostEstimate(flops=1_000_000_000, bytes_accessed=0, transcendentals=0),
        name="product",
    )(*parts, matrix)


def halves_kernel(first_ref, second_ref, first_half_ref, second_half_ref):
    half = first_half_ref.shape[1]
    first_half_ref[...] = first_ref[:, :half]
    second_half_ref[...] = second_ref[:, half:]


def halves(first, second):
    vmem = pl.BlockSpec(memory_space=pltpu.VMEM)
    half = jax.ShapeDtypeStruct((first.shape[0], first.shape[1] // 2), first.dtype)
    return pl.pallas_call(
        halves_kernel,
        out_shape=(half, half),
        in_specs=[vmem, vmem],
        out_specs=(vmem, vmem),
        compiler_params=pltpu.CompilerParams(vmem_limit_bytes=2**20),
        name="halves",
    )(first, second)


def epilogue_kernel(places, steps, *refs):
    pieces = refs[: len(places)]
    counts_ref, shift_ref, gumbel_ref, par_ref = refs[len(places) : len(places) + 4]
    scores_ref, stats_ref, logits_ref, columns_ref, ring_ref = refs[len(places) + 4 :]
    batch_rows, width = counts_ref.shape
    place = lax.axis_index("vocab")
    y = lax.shift_right_logical(place, 4)
    z = jnp.bitwise_and(lax.shift_right_logical(place, 1), NZ - 1)
    c = jnp.bitwise_and(place, 1)
    where_is = {place: (ref, g) for ref, group in zip(pieces, places) for g, place in enumerate(group)}
    pair = 2
    ring = NZ * NC * pair
    for k, dy in enumerate((0, -1, 1, 2)):
        yy = jnp.bitwise_and(y + (dy + NY), NY - 1)
        for t in range(steps):
            for dz in range(NZ):
                block = []
                for dc in range(NC):
                    ref, g = where_is[dz, dc]
                    at = ((g * NY + k) * steps + t) * pair
                    block.append(ref[at : at + pair, :])
                row = dz * NC * pair + 8
                ring_ref[k * steps + t, row : row + pair, :] = jnp.where(c == 0, block[0], block[1])
                ring_ref[k * steps + t, row + pair : row + 2 * pair, :] = jnp.where(c == 0, block[1], block[0])
            ring_ref[k * steps + t, 4:8, :] = ring_ref[k * steps + t, ring + 4 : ring + 8, :]
            for i in range(ring // 8):
                even = ring_ref[k * steps + t, 8 * i + 8 : 8 * i + 16, :]
                odd = ring_ref[k * steps + t, 8 * i + 4 : 8 * i + 12, :]
                tile = jnp.bitwise_and(i + lax.shift_right_logical(z, 1), ring // 8 - 1)
                at = pl.multiple_of(yy * ring + tile * 8, 8)
                logits_ref[t, pl.ds(at, 8), :] = jnp.where(jnp.bitwise_and(z, 1) == 1, odd, even)

    rows_at_once = 32
    lane = lax.broadcasted_iota(jnp.int32, (rows_at_once, width), 1).astype(jnp.float32)

    def some_rows(i, carry):
        rows = pl.ds(pl.multiple_of(i * rows_at_once, rows_at_once), rows_at_once)
        par = par_ref[rows, :]
        repeat, unrepeat = par[:, 0:1], par[:, 1:2]
        present, frequent, cooling = par[:, 2:3], par[:, 3:4], par[:, 4:5]
        emitted = par[:, 8 : 8 + steps]
        counts = counts_ref[rows, :]
        shift = shift_ref[rows, :]
        for t in range(steps):
            biased = logits_ref[t, rows, :] + shift
            seen = counts > 0
            factor = jnp.where(biased > 0, unrepeat, repeat)
            charged = biased * jnp.where(seen, factor, 1.0)
            charged = charged - frequent * counts - jnp.where(seen, present, 0.0)
            scores = charged * cooling
            hit = lane == emitted[:, t : t + 1]
            top = jnp.max(scores, axis=1, keepdims=True)
            total = jnp.sum(jnp.exp(scores - top), axis=1, keepdims=True)
            columns_ref[rows, 3 * t : 3 * t + 1] = top + jnp.log(total)
            columns_ref[rows, 3 * t + 1 : 3 * t + 2] = jnp.max(
                scores + gumbel_ref[t, rows, :], axis=1, keepdims=True
            )
            columns_ref[rows, 3 * t + 2 : 3 * t + 3] = jnp.sum(
                jnp.where(hit, scores, 0.0), axis=1, keepdims=True
            )
            if t == steps - 1:
                scores_ref[rows, :] = scores
            counts = counts + jnp.where(hit, 1.0, 0.0)
        return carry

    lax.fori_loop(0, batch_rows // rows_at_once, some_rows, 0)
    turned = columns_ref[...].T[: 3 * steps, :]
    for k in range(NV):
        stats_ref[3 * steps * k : 3 * steps * (k + 1), :] = turned


def epilogue(places, pieces, counts, shift, gumbel, par):
    steps, batch_rows, width = gumbel.shape
    vmem = pl.BlockSpec(memory_space=pltpu.VMEM)
    return pl.pallas_call(
        functools.partial(epilogue_kernel, places, steps),
        out_shape=(
            jax.ShapeDtypeStruct((batch_rows, width), jnp.float32),
            jax.ShapeDtypeStruct((NV * 3 * steps, batch_rows), jnp.float32),
        ),
        in_specs=[vmem] * (len(pieces) + 4),
        out_specs=(vmem, vmem),
        scratch_shapes=[
            pltpu.VMEM((steps, batch_rows, width), jnp.float32),
            pltpu.VMEM((batch_rows, LANES), jnp.float32),
            pltpu.VMEM((NY * steps, NZ * NC * 2 + 8, width), jnp.float32),
        ],
        compiler_params=pltpu.CompilerParams(vmem_limit_bytes=8 * 2**20),
        cost_estimate=pl.CostEstimate(flops=2_000_000_000, bytes_accessed=4_000_000, transcendentals=200_000),
        name="epilogue",
    )(*pieces, counts, shift, gumbel, par)


def finish_kernel(everyone_ref, scores_ref, best_ref, target_ref, last_hbm, last_ref, sem):
    steps, batch_rows = best_ref.shape
    each = 3 * steps

    def stat(t, k):
        return everyone_ref[pl.ds(3 * t + k, NV, stride=each), :]

    for t in reversed(range(steps)):
        local = stat(t, 0)
        top = jnp.max(local, axis=0, keepdims=True)
        normalizer = top + jnp.log(jnp.sum(jnp.exp(local - top), axis=0, keepdims=True))
        if t == steps - 1:
            column = jnp.broadcast_to(normalizer, (batch_rows, batch_rows)).T
            for k in range(scores_ref.shape[1] // LANES):
                at = slice(k * LANES, (k + 1) * LANES)
                last_ref[:, at] = scores_ref[:, at] - column
            copy = pltpu.make_async_copy(last_ref, last_hbm, sem)
            copy.start()
        best_ref[t : t + 1, :] = jnp.max(stat(t, 1), axis=0, keepdims=True)
        target_ref[t : t + 1, :] = jnp.sum(stat(t, 2), axis=0, keepdims=True) - normalizer
    copy.wait()


def finish(everyone, scores, steps):
    batch_rows, width = scores.shape
    vmem = pl.BlockSpec(memory_space=pltpu.VMEM)
    small = jax.ShapeDtypeStruct((steps, batch_rows), jnp.float32)
    return pl.pallas_call(
        finish_kernel,
        out_shape=(small, small, jax.ShapeDtypeStruct((batch_rows, width), jnp.float32)),
        in_specs=[vmem, vmem],
        out_specs=(vmem, vmem, pl.BlockSpec(memory_space=pltpu.HBM)),
        scratch_shapes=[pltpu.VMEM((batch_rows, width), jnp.float32), pltpu.SemaphoreType.DMA],
        compiler_params=pltpu.CompilerParams(vmem_limit_bytes=4 * 2**20),
        name="finish",
    )(everyone, scores)


def gathered_products(own, matrix):
    dim = own.shape[-1]
    column = [own, moved(own, dy=1), moved(own, dy=-1), moved(own, dy=2)]
    bundle = jnp.concatenate(column, 0).reshape(-1, dim)
    other = moved(bundle, dc=1)
    products = [product([[bundle], [other]], matrix)]
    places = [[(0, 0), (0, 1)]]
    up, down = bundle, bundle
    for step in range(1, NZ // 2):
        up = moved(up, dz=1)
        down = moved(down, dz=-1)
        others = moved(up, dc=1), moved(down, dc=1)
        products.append(product([[up], [down], [others[0]], [others[1]]], matrix))
        places.append([(NZ - step, 0), (step, 0), (NZ - step, 1), (step, 1)])
    up, down = halves(up, down)
    up = moved(up, dz=1)
    down = moved(down, dz=-1)
    others = moved(up, dc=1), moved(down, dc=1)
    products.append(product([[up, down], list(others)], matrix))
    places.append([(NZ // 2, 0), (NZ // 2, 1)])
    return products, places


def statistics(
    latent_activation,
    readout_matrix,
    caller_additive_shift,
    uniform_jitter,
    context_word_indices,
    emitted_word_indices,
    heat_factor,
    recurrence_charge,
    appearance_charge,
    occurrence_charge,
):
    steps, batch_rows = uniform_jitter.shape[:2]
    counts, gumbel, par = prologue(
        context_word_indices,
        uniform_jitter,
        emitted_word_indices.T,
        recurrence_charge[None],
        appearance_charge[None],
        occurrence_charge[None],
        heat_factor[None],
    )
    products, places = gathered_products(latent_activation, readout_matrix)
    scores, stats = epilogue(places, products, counts, caller_additive_shift, gumbel, par)
    everyone = lax.all_to_all(
        stats.reshape(NV, 1, 3 * steps * batch_rows), "vocab", 0, 0, tiled=True
    ).reshape(stats.shape)
    return finish(everyone, scores, steps)


def solution(mesh):
    in_specs = (
        P(None, ("batch", "vocab"), None),
        P(None, "vocab"),
        P("batch", "vocab"),
        P(None, "batch", "vocab"),
        P("batch", None),
        P("batch", None),
        P("batch"),
        P("batch"),
        P("batch"),
        P("batch"),
    )
    out_specs = (P(None, "batch"), P(None, "batch"), P("batch", "vocab"))
    return jax.shard_map(statistics, mesh=mesh, in_specs=in_specs, out_specs=out_specs, check_vma=False)
```

```python
import functools

import jax
import jax.numpy as jnp
from jax import lax
from jax.experimental import pallas as pl
from jax.experimental.pallas import tpu as pltpu
from jax.sharding import PartitionSpec as P


NY, NZ, NC = 4, 8, 2
LANES = 128


def device_of(y, z, c):
    return ((y % NY) * NZ + z % NZ) * NC + c % NC


def moved(array, dy=0, dz=0, dc=0):
    pairs = [
        (device_of(y, z, c), device_of(y + dy, z + dz, c + dc))
        for y in range(NY)
        for z in range(NZ)
        for c in range(NC)
    ]
    return lax.ppermute(array, "vocab", pairs)


def noise_kernel(jitter_ref, own_ref, given_ref, gumbel_ref, kept_ref, par_ref, rows_ref):
    steps, batch_rows, width = gumbel_ref.shape
    kept_ref[...] = own_ref[...]
    base = (lax.axis_index("vocab") * width).astype(jnp.float32)
    rows_ref[...] = jnp.zeros_like(rows_ref)
    rows_ref[0:4, :] = given_ref[0:4, :]
    rows_ref[4:5, :] = 1.0 / given_ref[0:1, :]
    rows_ref[5:6, :] = 1.0 / given_ref[3:4, :]
    rows_ref[8 : 8 + steps, :] = given_ref[4 : 4 + steps, :] - base
    par_ref[...] = rows_ref[...].T

    def some_rows(i, carry):
        rows = pl.ds(pl.multiple_of(i * 16, 16), 16)
        for t in range(steps):
            gumbel_ref[t, rows, :] = -jnp.log(-jnp.log(jitter_ref[t, rows, :]))
        return carry

    lax.fori_loop(0, batch_rows // 16, some_rows, 0)


def noise(jitter, own, given):
    vmem = pl.BlockSpec(memory_space=pltpu.VMEM)
    return pl.pallas_call(
        noise_kernel,
        out_shape=(
            jax.ShapeDtypeStruct(jitter.shape, jnp.float32),
            jax.ShapeDtypeStruct(own.shape, own.dtype),
            jax.ShapeDtypeStruct((jitter.shape[1], LANES), jnp.float32),
        ),
        in_specs=[vmem, vmem, vmem],
        out_specs=(vmem, vmem, vmem),
        scratch_shapes=[pltpu.VMEM((LANES, jitter.shape[1]), jnp.float32)],
        compiler_params=pltpu.CompilerParams(vmem_limit_bytes=2 * 2**20),
        cost_estimate=pl.CostEstimate(flops=2_000_000_000, bytes_accessed=2_000_000, transcendentals=800_000),
        name="noise",
    )(jitter, own, given)


def counts_kernel(ctx_ref, counts_ref, found_ref):
    batch_rows, length = ctx_ref.shape
    width = counts_ref.shape[1]
    blocks = width // LANES
    base = lax.axis_index("vocab") * width
    block_ids = lax.broadcasted_iota(jnp.int32, (8, length), 0)
    lane_ids = lax.broadcasted_iota(jnp.int32, (LANES, length), 0)

    def count_row(b):
        local = ctx_ref[pl.ds(b, 1), :] - base
        high = lax.shift_right_arithmetic(local, 7)
        low = jnp.bitwise_and(local, LANES - 1)
        lhs = (block_ids == high).astype(jnp.float32).astype(jnp.bfloat16)
        rhs = (lane_ids == low).astype(jnp.float32).astype(jnp.bfloat16)
        return lax.dot_general(lhs, rhs, (((1,), (1,)), ((), ())), preferred_element_type=jnp.float32)

    def count_rows(i, carry):
        rows = pl.ds(pl.multiple_of(i * 8, 8), 8)
        for j in range(8):
            found_ref[8 * j : 8 * j + 8, :] = count_row(i * 8 + j)
        for k in range(blocks):
            counts_ref[rows, k * LANES : (k + 1) * LANES] = found_ref[pl.ds(k, 8, stride=8), :]
        return carry

    lax.fori_loop(0, batch_rows // 8, count_rows, 0)


def counts_of(ctx, width):
    vmem = pl.BlockSpec(memory_space=pltpu.VMEM)
    return pl.pallas_call(
        counts_kernel,
        out_shape=jax.ShapeDtypeStruct((ctx.shape[0], width), jnp.float32),
        in_specs=[vmem],
        out_specs=vmem,
        scratch_shapes=[pltpu.VMEM((8 * 8, LANES), jnp.float32)],
        compiler_params=pltpu.CompilerParams(vmem_limit_bytes=2 * 2**20),
        cost_estimate=pl.CostEstimate(flops=5_000_000_000, bytes_accessed=400_000, transcendentals=0),
        name="counts",
    )(ctx)


def product_kernel(groups, *refs):
    matrix_ref, out_ref, rows_ref = refs[sum(groups) :]
    depth = 1024
    first = 0
    for g, parts in enumerate(groups):
        at = 0
        for ref in refs[first : first + parts]:
            count, part = ref.shape
            rows_ref[g * count : (g + 1) * count, at : at + part] = ref[...]
            at += part
        first += parts

    def add(k, carry):
        at = pl.ds(pl.multiple_of(k * depth, depth), depth)
        out_ref[...] += jnp.dot(rows_ref[:, at], matrix_ref[at, :], preferred_element_type=jnp.float32)
        return carry

    out_ref[...] = jnp.zeros_like(out_ref)
    lax.fori_loop(0, rows_ref.shape[1] // depth, add, 0)


def product(groups, matrix):
    vmem = pl.BlockSpec(memory_space=pltpu.VMEM)
    dim, width = matrix.shape
    count = sum(group[0].shape[0] for group in groups)
    parts = [part for group in groups for part in group]
    return pl.pallas_call(
        functools.partial(product_kernel, [len(group) for group in groups]),
        out_shape=jax.ShapeDtypeStruct((count, width), jnp.float32),
        in_specs=[vmem] * (len(parts) + 1),
        out_specs=vmem,
        scratch_shapes=[pltpu.VMEM((count, dim), jnp.bfloat16)],
        compiler_params=pltpu.CompilerParams(vmem_limit_bytes=4 * 2**20),
        cost_estimate=pl.CostEstimate(flops=1_000_000_000, bytes_accessed=0, transcendentals=0),
        name="product",
    )(*parts, matrix)


def halves_kernel(first_ref, second_ref, first_half_ref, second_half_ref):
    half = first_half_ref.shape[1]
    first_half_ref[...] = first_ref[:, :half]
    second_half_ref[...] = second_ref[:, half:]


def halves(first, second):
    vmem = pl.BlockSpec(memory_space=pltpu.VMEM)
    half = jax.ShapeDtypeStruct((first.shape[0], first.shape[1] // 2), first.dtype)
    return pl.pallas_call(
        halves_kernel,
        out_shape=(half, half),
        in_specs=[vmem, vmem],
        out_specs=(vmem, vmem),
        compiler_params=pltpu.CompilerParams(vmem_limit_bytes=2**20),
        name="halves",
    )(first, second)


def epilogue_kernel(places, steps, *refs):
    pieces = refs[: len(places)]
    counts_ref, shift_ref, gumbel_ref, par_ref = refs[len(places) : len(places) + 4]
    scores_ref, stats_ref, logits_ref, columns_ref, ring_ref = refs[len(places) + 4 :]
    batch_rows, width = counts_ref.shape
    place = lax.axis_index("vocab")
    y = lax.shift_right_logical(place, 4)
    z = jnp.bitwise_and(lax.shift_right_logical(place, 1), NZ - 1)
    c = jnp.bitwise_and(place, 1)
    where_is = {place: (ref, g) for ref, group in zip(pieces, places) for g, place in enumerate(group)}
    pair = 2
    ring = NZ * NC * pair
    for k, dy in enumerate((0, -1, 1, 2)):
        yy = jnp.bitwise_and(y + (dy + NY), NY - 1)
        for t in range(steps):
            for dz in range(NZ):
                block = []
                for dc in range(NC):
                    ref, g = where_is[dz, dc]
                    at = ((g * NY + k) * steps + t) * pair
                    block.append(ref[at : at + pair, :])
                row = dz * NC * pair + 8
                ring_ref[k * steps + t, row : row + pair, :] = jnp.where(c == 0, block[0], block[1])
                ring_ref[k * steps + t, row + pair : row + 2 * pair, :] = jnp.where(c == 0, block[1], block[0])
            ring_ref[k * steps + t, 4:8, :] = ring_ref[k * steps + t, ring + 4 : ring + 8, :]
            for i in range(ring // 8):
                even = ring_ref[k * steps + t, 8 * i + 8 : 8 * i + 16, :]
                odd = ring_ref[k * steps + t, 8 * i + 4 : 8 * i + 12, :]
                tile = jnp.bitwise_and(i + lax.shift_right_logical(z, 1), ring // 8 - 1)
                at = pl.multiple_of(yy * ring + tile * 8, 8)
                logits_ref[t, pl.ds(at, 8), :] = jnp.where(jnp.bitwise_and(z, 1) == 1, odd, even)

    rows_at_once = 32
    lane = lax.broadcasted_iota(jnp.int32, (rows_at_once, width), 1).astype(jnp.float32)

    def some_rows(i, carry):
        rows = pl.ds(pl.multiple_of(i * rows_at_once, rows_at_once), rows_at_once)
        par = par_ref[rows, :]
        repeat, unrepeat = par[:, 0:1], par[:, 4:5]
        present, frequent, cooling = par[:, 1:2], par[:, 2:3], par[:, 5:6]
        emitted = par[:, 8 : 8 + steps]
        counts = counts_ref[rows, :]
        shift = shift_ref[rows, :]
        for t in range(steps):
            biased = logits_ref[t, rows, :] + shift
            seen = counts > 0
            factor = jnp.where(biased > 0, unrepeat, repeat)
            charged = biased * jnp.where(seen, factor, 1.0)
            charged = charged - frequent * counts - jnp.where(seen, present, 0.0)
            scores = charged * cooling
            hit = lane == emitted[:, t : t + 1]
            top = jnp.max(scores, axis=1, keepdims=True)
            total = jnp.sum(jnp.exp(scores - top), axis=1, keepdims=True)
            columns_ref[rows, 3 * t : 3 * t + 1] = top + jnp.log(total)
            columns_ref[rows, 3 * t + 1 : 3 * t + 2] = jnp.max(
                scores + gumbel_ref[t, rows, :], axis=1, keepdims=True
            )
            columns_ref[rows, 3 * t + 2 : 3 * t + 3] = jnp.sum(
                jnp.where(hit, scores, 0.0), axis=1, keepdims=True
            )
            if t == steps - 1:
                scores_ref[rows, :] = scores
            counts = counts + jnp.where(hit, 1.0, 0.0)
        return carry

    lax.fori_loop(0, batch_rows // rows_at_once, some_rows, 0)
    stats_ref[...] = columns_ref[...].T[:16, :]


def epilogue(places, pieces, counts, shift, gumbel, par):
    steps, batch_rows, width = gumbel.shape
    vmem = pl.BlockSpec(memory_space=pltpu.VMEM)
    return pl.pallas_call(
        functools.partial(epilogue_kernel, places, steps),
        out_shape=(
            jax.ShapeDtypeStruct((batch_rows, width), jnp.float32),
            jax.ShapeDtypeStruct((16, batch_rows), jnp.float32),
        ),
        in_specs=[vmem] * (len(pieces) + 4),
        out_specs=(vmem, vmem),
        scratch_shapes=[
            pltpu.VMEM((steps, batch_rows, width), jnp.float32),
            pltpu.VMEM((batch_rows, LANES), jnp.float32),
            pltpu.VMEM((NY * steps, NZ * NC * 2 + 8, width), jnp.float32),
        ],
        compiler_params=pltpu.CompilerParams(vmem_limit_bytes=8 * 2**20),
        cost_estimate=pl.CostEstimate(flops=2_000_000_000, bytes_accessed=4_000_000, transcendentals=200_000),
        name="epilogue",
    )(*pieces, counts, shift, gumbel, par)


def merge_kernel(steps, mine_ref, other_ref, out_ref):
    each = 3 * steps
    mine, other = mine_ref[:each, :], other_ref[:each, :]
    kind = lax.broadcasted_iota(jnp.int32, mine.shape, 0) % 3
    top = jnp.maximum(mine, other)
    either = top + jnp.log(jnp.exp(mine - top) + jnp.exp(other - top))
    both = jnp.where(kind == 0, either, jnp.where(kind == 1, top, mine + other))
    for k in range(out_ref.shape[0] // each):
        out_ref[each * k : each * (k + 1), :] = both


def merge(mine, other, steps, copies):
    vmem = pl.BlockSpec(memory_space=pltpu.VMEM)
    return pl.pallas_call(
        functools.partial(merge_kernel, steps),
        out_shape=jax.ShapeDtypeStruct((copies * 3 * steps, mine.shape[1]), jnp.float32),
        in_specs=[vmem, vmem],
        out_specs=vmem,
        compiler_params=pltpu.CompilerParams(vmem_limit_bytes=2**20),
        name="merge",
    )(mine, other)


def finish_kernel(everyone_ref, scores_ref, best_ref, target_ref, last_hbm, last_ref, sem):
    steps, batch_rows = best_ref.shape
    each = 3 * steps

    def stat(t, k):
        return everyone_ref[pl.ds(3 * t + k, everyone_ref.shape[0] // each, stride=each), :]

    for t in reversed(range(steps)):
        local = stat(t, 0)
        top = jnp.max(local, axis=0, keepdims=True)
        normalizer = top + jnp.log(jnp.sum(jnp.exp(local - top), axis=0, keepdims=True))
        if t == steps - 1:
            column = jnp.broadcast_to(normalizer, (batch_rows, batch_rows)).T
            for k in range(scores_ref.shape[1] // LANES):
                at = slice(k * LANES, (k + 1) * LANES)
                last_ref[:, at] = scores_ref[:, at] - column
            copy = pltpu.make_async_copy(last_ref, last_hbm, sem)
            copy.start()
        best_ref[t : t + 1, :] = jnp.max(stat(t, 1), axis=0, keepdims=True)
        target_ref[t : t + 1, :] = jnp.sum(stat(t, 2), axis=0, keepdims=True) - normalizer
    copy.wait()


def finish(everyone, scores, steps):
    batch_rows, width = scores.shape
    vmem = pl.BlockSpec(memory_space=pltpu.VMEM)
    small = jax.ShapeDtypeStruct((steps, batch_rows), jnp.float32)
    return pl.pallas_call(
        finish_kernel,
        out_shape=(small, small, jax.ShapeDtypeStruct((batch_rows, width), jnp.float32)),
        in_specs=[vmem, vmem],
        out_specs=(vmem, vmem, pl.BlockSpec(memory_space=pltpu.HBM)),
        scratch_shapes=[pltpu.VMEM((batch_rows, width), jnp.float32), pltpu.SemaphoreType.DMA],
        compiler_params=pltpu.CompilerParams(vmem_limit_bytes=4 * 2**20),
        name="finish",
    )(everyone, scores)


def gathered_products(own, kept, matrix):
    dim = own.shape[-1]
    column = []
    for dy in (1, -1, 2):
        column.append(moved(own, dy=dy))
    bundle = jnp.concatenate([kept, *column], 0).reshape(-1, dim)
    other = moved(bundle, dc=1)
    products = [product([[bundle], [other]], matrix)]
    places = [[(0, 0), (0, 1)]]
    up, down = bundle, bundle
    for step in range(1, NZ // 2):
        up = moved(up, dz=1)
        down = moved(down, dz=-1)
        others = moved(up, dc=1), moved(down, dc=1)
        products.append(product([[up], [down], [others[0]], [others[1]]], matrix))
        places.append([(NZ - step, 0), (step, 0), (NZ - step, 1), (step, 1)])
    up, down = halves(up, down)
    up = moved(up, dz=1)
    down = moved(down, dz=-1)
    others = moved(up, dc=1), moved(down, dc=1)
    products.append(product([[up, down], list(others)], matrix))
    places.append([(NZ // 2, 0), (NZ // 2, 1)])
    return products, places


def statistics(
    latent_activation,
    readout_matrix,
    caller_additive_shift,
    uniform_jitter,
    context_word_indices,
    emitted_word_indices,
    heat_factor,
    recurrence_charge,
    appearance_charge,
    occurrence_charge,
):
    steps, batch_rows = uniform_jitter.shape[:2]
    width = readout_matrix.shape[1]
    given = jnp.concatenate(
        [
            jnp.stack([recurrence_charge, appearance_charge, occurrence_charge, heat_factor]),
            emitted_word_indices.T.astype(jnp.float32),
        ]
    )
    gumbel, kept, par = noise(uniform_jitter, latent_activation, given)
    counts = counts_of(context_word_indices, width)
    products, places = gathered_products(latent_activation, kept, readout_matrix)
    scores, stats = epilogue(places, products, counts, caller_additive_shift, gumbel, par)
    merged = merge(stats, moved(stats, dc=1), steps, NY * NZ)
    groups = [[device_of(y, z, c) for y in range(NY) for z in range(NZ)] for c in range(NC)]
    everyone = lax.all_to_all(
        merged.reshape(NY * NZ, 1, 3 * steps * batch_rows),
        "vocab",
        0,
        0,
        axis_index_groups=groups,
        tiled=True,
    ).reshape(merged.shape)
    return finish(everyone, scores, steps)


def solution(mesh):
    in_specs = (
        P(None, ("batch", "vocab"), None),
        P(None, "vocab"),
        P("batch", "vocab"),
        P(None, "batch", "vocab"),
        P("batch", None),
        P("batch", None),
        P("batch"),
        P("batch"),
        P("batch"),
        P("batch"),
    )
    out_specs = (P(None, "batch"), P(None, "batch"), P("batch", "vocab"))
    return jax.shard_map(statistics, mesh=mesh, in_specs=in_specs, out_specs=out_specs, check_vma=False)
```

```python
import functools

import jax
import jax.numpy as jnp
from jax import lax
from jax.experimental import pallas as pl
from jax.experimental.pallas import tpu as pltpu
from jax.sharding import PartitionSpec as P


NY, NZ, NC = 4, 8, 2
LANES = 128


PARTS = 2


def device_of(y, z, c):
    return ((y % NY) * NZ + z % NZ) * NC + c % NC


def moved(array, dy=0, dz=0, dc=0):
    pairs = [
        (device_of(y, z, c), device_of(y + dy, z + dz, c + dc))
        for y in range(NY)
        for z in range(NZ)
        for c in range(NC)
    ]
    return lax.ppermute(array, "vocab", pairs)


def passed_on(array):
    pairs = [
        (device_of(y, z, c), device_of(y, z + 1 - 2 * c, c))
        for y in range(NY)
        for z in range(NZ)
        for c in range(NC)
    ]
    return lax.ppermute(array, "vocab", pairs)


def noise_kernel(jitter_ref, own_ref, given_ref, gumbel_ref, kept_ref, par_ref, rows_ref):
    steps, batch_rows, width = gumbel_ref.shape
    kept_ref[...] = own_ref[...]
    base = (lax.axis_index("vocab") * width).astype(jnp.float32)
    rows_ref[...] = jnp.zeros_like(rows_ref)
    rows_ref[0:4, :] = given_ref[0:4, :]
    rows_ref[4:5, :] = 1.0 / given_ref[0:1, :]
    rows_ref[5:6, :] = 1.0 / given_ref[3:4, :]
    rows_ref[8 : 8 + steps, :] = given_ref[4 : 4 + steps, :] - base
    par_ref[...] = rows_ref[...].T

    def some_rows(i, carry):
        rows = pl.ds(pl.multiple_of(i * 16, 16), 16)
        for t in range(steps):
            gumbel_ref[t, rows, :] = -jnp.log(-jnp.log(jitter_ref[t, rows, :]))
        return carry

    lax.fori_loop(0, batch_rows // 16, some_rows, 0)


def noise(jitter, own, given):
    vmem = pl.BlockSpec(memory_space=pltpu.VMEM)
    return pl.pallas_call(
        noise_kernel,
        out_shape=(
            jax.ShapeDtypeStruct(jitter.shape, jnp.float32),
            jax.ShapeDtypeStruct(own.shape, own.dtype),
            jax.ShapeDtypeStruct((jitter.shape[1], LANES), jnp.float32),
        ),
        in_specs=[vmem, vmem, vmem],
        out_specs=(vmem, vmem, vmem),
        scratch_shapes=[pltpu.VMEM((LANES, jitter.shape[1]), jnp.float32)],
        compiler_params=pltpu.CompilerParams(vmem_limit_bytes=2 * 2**20),
        cost_estimate=pl.CostEstimate(flops=2_000_000_000, bytes_accessed=2_000_000, transcendentals=800_000),
        name="noise",
    )(jitter, own, given)


def counts_kernel(ctx_ref, counts_ref, found_ref):
    batch_rows, length = ctx_ref.shape
    width = counts_ref.shape[1]
    blocks = width // LANES
    base = lax.axis_index("vocab") * width
    block_ids = lax.broadcasted_iota(jnp.int32, (8, length), 0)
    lane_ids = lax.broadcasted_iota(jnp.int32, (LANES, length), 0)

    def count_row(b):
        local = ctx_ref[pl.ds(b, 1), :] - base
        high = lax.shift_right_arithmetic(local, 7)
        low = jnp.bitwise_and(local, LANES - 1)
        lhs = (block_ids == high).astype(jnp.float32).astype(jnp.bfloat16)
        rhs = (lane_ids == low).astype(jnp.float32).astype(jnp.bfloat16)
        return lax.dot_general(lhs, rhs, (((1,), (1,)), ((), ())), preferred_element_type=jnp.float32)

    def count_rows(i, carry):
        rows = pl.ds(pl.multiple_of(i * 8, 8), 8)
        for j in range(8):
            found_ref[8 * j : 8 * j + 8, :] = count_row(i * 8 + j)
        for k in range(blocks):
            counts_ref[rows, k * LANES : (k + 1) * LANES] = found_ref[pl.ds(k, 8, stride=8), :]
        return carry

    lax.fori_loop(0, batch_rows // 8, count_rows, 0)


def counts_of(ctx, width):
    vmem = pl.BlockSpec(memory_space=pltpu.VMEM)
    return pl.pallas_call(
        counts_kernel,
        out_shape=jax.ShapeDtypeStruct((ctx.shape[0], width), jnp.float32),
        in_specs=[vmem],
        out_specs=vmem,
        scratch_shapes=[pltpu.VMEM((8 * 8, LANES), jnp.float32)],
        compiler_params=pltpu.CompilerParams(vmem_limit_bytes=2 * 2**20),
        cost_estimate=pl.CostEstimate(flops=5_000_000_000, bytes_accessed=400_000, transcendentals=0),
        name="counts",
    )(ctx)


def product_kernel(groups, *refs):
    matrix_ref, out_ref, rows_ref = refs[sum(groups) :]
    depth = 1024
    first = 0
    for g, parts in enumerate(groups):
        at = 0
        for ref in refs[first : first + parts]:
            count, part = ref.shape
            rows_ref[g * count : (g + 1) * count, at : at + part] = ref[...]
            at += part
        first += parts

    def add(k, carry):
        at = pl.ds(pl.multiple_of(k * depth, depth), depth)
        out_ref[...] += jnp.dot(rows_ref[:, at], matrix_ref[at, :], preferred_element_type=jnp.float32)
        return carry

    out_ref[...] = jnp.zeros_like(out_ref)
    lax.fori_loop(0, rows_ref.shape[1] // depth, add, 0)


def product(groups, matrix):
    vmem = pl.BlockSpec(memory_space=pltpu.VMEM)
    dim, width = matrix.shape
    count = sum(group[0].shape[0] for group in groups)
    parts = [part for group in groups for part in group]
    return pl.pallas_call(
        functools.partial(product_kernel, [len(group) for group in groups]),
        out_shape=jax.ShapeDtypeStruct((count, width), jnp.float32),
        in_specs=[vmem] * (len(parts) + 1),
        out_specs=vmem,
        scratch_shapes=[pltpu.VMEM((count, dim), jnp.bfloat16)],
        compiler_params=pltpu.CompilerParams(vmem_limit_bytes=4 * 2**20),
        cost_estimate=pl.CostEstimate(flops=1_000_000_000, bytes_accessed=0, transcendentals=0),
        name="product",
    )(*parts, matrix)


def bundle_kernel(*refs):
    outs = refs[NY:]
    part = outs[0].shape[1]
    for k, ref in enumerate(refs[:NY]):
        steps, pair = ref.shape[:2]
        for t in range(steps):
            row = (k * steps + t) * pair
            for g, out in enumerate(outs):
                out[row : row + pair, :] = ref[t, :, g * part : (g + 1) * part]


def bundle_of(column, parts):
    vmem = pl.BlockSpec(memory_space=pltpu.VMEM)
    steps, pair, dim = column[0].shape
    out = jax.ShapeDtypeStruct((len(column) * steps * pair, dim // parts), column[0].dtype)
    return pl.pallas_call(
        bundle_kernel,
        out_shape=(out,) * parts,
        in_specs=[vmem] * len(column),
        out_specs=(vmem,) * parts,
        compiler_params=pltpu.CompilerParams(vmem_limit_bytes=2**20),
        name="bundle",
    )(*column)


def epilogue_kernel(places, steps, *refs):
    pieces = refs[: len(places)]
    counts_ref, shift_ref, gumbel_ref, par_ref = refs[len(places) : len(places) + 4]
    scores_ref, stats_ref, logits_ref, columns_ref, ring_ref = refs[len(places) + 4 :]
    batch_rows, width = counts_ref.shape
    place = lax.axis_index("vocab")
    y = lax.shift_right_logical(place, 4)
    z = jnp.bitwise_and(lax.shift_right_logical(place, 1), NZ - 1)
    c = jnp.bitwise_and(place, 1)
    where_is = {name: (ref, g) for ref, group in zip(pieces, places) for g, name in enumerate(group)}
    pair = 2
    ring = NZ * NC * pair

    def named(dz, core, of):
        dc = core ^ of
        if dz == 0:
            return "own", 0, dc
        if dz == NZ // 2:
            return ("passed" if dc == 0 else "swapped"), dz, dc
        up = dz > NZ // 2
        return ("passed" if up == (of == 0) else "swapped"), min(dz, NZ - dz), dc

    for k, dy in enumerate((0, -1, 1, 2)):
        yy = jnp.bitwise_and(y + (dy + NY), NY - 1)
        for t in range(steps):
            for dz in range(NZ):
                for core in range(NC):
                    values = []
                    for of in range(NC):
                        ref, g = where_is[named(dz, core, of)]
                        at = ((g * NY + k) * steps + t) * pair
                        values.append(ref[at : at + pair, :])
                    row = (dz * NC + core) * pair + 8
                    ring_ref[k * steps + t, row : row + pair, :] = jnp.where(c == 0, *values)
            ring_ref[k * steps + t, 4:8, :] = ring_ref[k * steps + t, ring + 4 : ring + 8, :]
            for i in range(ring // 8):
                even = ring_ref[k * steps + t, 8 * i + 8 : 8 * i + 16, :]
                odd = ring_ref[k * steps + t, 8 * i + 4 : 8 * i + 12, :]
                tile = jnp.bitwise_and(i + lax.shift_right_logical(z, 1), ring // 8 - 1)
                at = pl.multiple_of(yy * ring + tile * 8, 8)
                logits_ref[t, pl.ds(at, 8), :] = jnp.where(jnp.bitwise_and(z, 1) == 1, odd, even)

    rows_at_once = 32
    lane = lax.broadcasted_iota(jnp.int32, (rows_at_once, width), 1).astype(jnp.float32)

    def some_rows(i, carry):
        rows = pl.ds(pl.multiple_of(i * rows_at_once, rows_at_once), rows_at_once)
        par = par_ref[rows, :]
        repeat, unrepeat = par[:, 0:1], par[:, 4:5]
        present, frequent, cooling = par[:, 1:2], par[:, 2:3], par[:, 5:6]
        emitted = par[:, 8 : 8 + steps]
        counts = counts_ref[rows, :]
        shift = shift_ref[rows, :]
        for t in range(steps):
            biased = logits_ref[t, rows, :] + shift
            seen = counts > 0
            factor = jnp.where(biased > 0, unrepeat, repeat)
            charged = biased * jnp.where(seen, factor, 1.0)
            charged = charged - frequent * counts - jnp.where(seen, present, 0.0)
            scores = charged * cooling
            hit = lane == emitted[:, t : t + 1]
            top = jnp.max(scores, axis=1, keepdims=True)
            total = jnp.sum(jnp.exp(scores - top), axis=1, keepdims=True)
            columns_ref[rows, 3 * t : 3 * t + 1] = top + jnp.log(total)
            columns_ref[rows, 3 * t + 1 : 3 * t + 2] = jnp.max(
                scores + gumbel_ref[t, rows, :], axis=1, keepdims=True
            )
            columns_ref[rows, 3 * t + 2 : 3 * t + 3] = jnp.sum(
                jnp.where(hit, scores, 0.0), axis=1, keepdims=True
            )
            if t == steps - 1:
                scores_ref[rows, :] = scores
            counts = counts + jnp.where(hit, 1.0, 0.0)
        return carry

    lax.fori_loop(0, batch_rows // rows_at_once, some_rows, 0)
    stats_ref[...] = columns_ref[...].T[:16, :]


def epilogue(places, pieces, counts, shift, gumbel, par):
    steps, batch_rows, width = gumbel.shape
    vmem = pl.BlockSpec(memory_space=pltpu.VMEM)
    return pl.pallas_call(
        functools.partial(epilogue_kernel, places, steps),
        out_shape=(
            jax.ShapeDtypeStruct((batch_rows, width), jnp.float32),
            jax.ShapeDtypeStruct((16, batch_rows), jnp.float32),
        ),
        in_specs=[vmem] * (len(pieces) + 4),
        out_specs=(vmem, vmem),
        scratch_shapes=[
            pltpu.VMEM((steps, batch_rows, width), jnp.float32),
            pltpu.VMEM((batch_rows, LANES), jnp.float32),
            pltpu.VMEM((NY * steps, NZ * NC * 2 + 8, width), jnp.float32),
        ],
        compiler_params=pltpu.CompilerParams(vmem_limit_bytes=8 * 2**20),
        cost_estimate=pl.CostEstimate(flops=2_000_000_000, bytes_accessed=4_000_000, transcendentals=200_000),
        name="epilogue",
    )(*pieces, counts, shift, gumbel, par)


def merge_kernel(steps, mine_ref, other_ref, out_ref):
    each = 3 * steps
    mine, other = mine_ref[:each, :], other_ref[:each, :]
    kind = lax.broadcasted_iota(jnp.int32, mine.shape, 0) % 3
    top = jnp.maximum(mine, other)
    either = top + jnp.log(jnp.exp(mine - top) + jnp.exp(other - top))
    both = jnp.where(kind == 0, either, jnp.where(kind == 1, top, mine + other))
    for k in range(out_ref.shape[0] // each):
        out_ref[each * k : each * (k + 1), :] = both


def merge(mine, other, steps, copies):
    vmem = pl.BlockSpec(memory_space=pltpu.VMEM)
    return pl.pallas_call(
        functools.partial(merge_kernel, steps),
        out_shape=jax.ShapeDtypeStruct((copies * 3 * steps, mine.shape[1]), jnp.float32),
        in_specs=[vmem, vmem],
        out_specs=vmem,
        compiler_params=pltpu.CompilerParams(vmem_limit_bytes=2**20),
        name="merge",
    )(mine, other)


def finish_kernel(everyone_ref, scores_ref, best_ref, target_ref, last_hbm, last_ref, sem):
    steps, batch_rows = best_ref.shape
    each = 3 * steps

    def stat(t, k):
        return everyone_ref[pl.ds(3 * t + k, everyone_ref.shape[0] // each, stride=each), :]

    for t in reversed(range(steps)):
        local = stat(t, 0)
        top = jnp.max(local, axis=0, keepdims=True)
        normalizer = top + jnp.log(jnp.sum(jnp.exp(local - top), axis=0, keepdims=True))
        if t == steps - 1:
            column = jnp.broadcast_to(normalizer, (batch_rows, batch_rows)).T
            for k in range(scores_ref.shape[1] // LANES):
                at = slice(k * LANES, (k + 1) * LANES)
                last_ref[:, at] = scores_ref[:, at] - column
            copy = pltpu.make_async_copy(last_ref, last_hbm, sem)
            copy.start()
        best_ref[t : t + 1, :] = jnp.max(stat(t, 1), axis=0, keepdims=True)
        target_ref[t : t + 1, :] = jnp.sum(stat(t, 2), axis=0, keepdims=True) - normalizer
    copy.wait()


def finish(everyone, scores, steps):
    batch_rows, width = scores.shape
    vmem = pl.BlockSpec(memory_space=pltpu.VMEM)
    small = jax.ShapeDtypeStruct((steps, batch_rows), jnp.float32)
    return pl.pallas_call(
        finish_kernel,
        out_shape=(small, small, jax.ShapeDtypeStruct((batch_rows, width), jnp.float32)),
        in_specs=[vmem, vmem],
        out_specs=(vmem, vmem, pl.BlockSpec(memory_space=pltpu.HBM)),
        scratch_shapes=[pltpu.VMEM((batch_rows, width), jnp.float32), pltpu.SemaphoreType.DMA],
        compiler_params=pltpu.CompilerParams(vmem_limit_bytes=4 * 2**20),
        name="finish",
    )(everyone, scores)


def in_parts(move, parts):
    moves = []
    for part in parts:
        moves.append(move(part))
    return moves


def gathered_products(own, kept, matrix):
    swapped = functools.partial(moved, dc=1)
    column = []
    for dy in (1, -1, 2):
        column.append(moved(own, dy=dy))
    mine = bundle_of([kept, *column], PARTS)
    other = in_parts(swapped, mine)
    groups = [mine, other]
    names = [("own", 0, 0), ("own", 0, 1)]
    products, places = [], []
    for step in range(1, NZ // 2 + 1):
        mine = in_parts(passed_on, mine)
        groups += [mine, in_parts(swapped, mine)]
        names += [("passed", step, 0), ("swapped", step, 1)]
        if step < NZ // 2:
            other = in_parts(passed_on, other)
            groups += [other, in_parts(swapped, other)]
            names += [("passed", step, 1), ("swapped", step, 0)]
        products.append(product(groups, matrix))
        places.append(names)
        groups, names = [], []
    return products, places


def statistics(
    latent_activation,
    readout_matrix,
    caller_additive_shift,
    uniform_jitter,
    context_word_indices,
    emitted_word_indices,
    heat_factor,
    recurrence_charge,
    appearance_charge,
    occurrence_charge,
):
    steps, batch_rows = uniform_jitter.shape[:2]
    width = readout_matrix.shape[1]
    given = jnp.concatenate(
        [
            jnp.stack([recurrence_charge, appearance_charge, occurrence_charge, heat_factor]),
            emitted_word_indices.T.astype(jnp.float32),
        ]
    )
    gumbel, kept, par = noise(uniform_jitter, latent_activation, given)
    counts = counts_of(context_word_indices, width)
    products, places = gathered_products(latent_activation, kept, readout_matrix)
    scores, stats = epilogue(places, products, counts, caller_additive_shift, gumbel, par)
    merged = merge(stats, moved(stats, dc=1), steps, NY * NZ)
    groups = [[device_of(y, z, c) for y in range(NY) for z in range(NZ)] for c in range(NC)]
    everyone = lax.all_to_all(
        merged.reshape(NY * NZ, 1, 3 * steps * batch_rows),
        "vocab",
        0,
        0,
        axis_index_groups=groups,
        tiled=True,
    ).reshape(merged.shape)
    return finish(everyone, scores, steps)


def solution(mesh):
    in_specs = (
        P(None, ("batch", "vocab"), None),
        P(None, "vocab"),
        P("batch", "vocab"),
        P(None, "batch", "vocab"),
        P("batch", None),
        P("batch", None),
        P("batch"),
        P("batch"),
        P("batch"),
        P("batch"),
    )
    out_specs = (P(None, "batch"), P(None, "batch"), P("batch", "vocab"))
    return jax.shard_map(statistics, mesh=mesh, in_specs=in_specs, out_specs=out_specs, check_vma=False)
```
